1024 devices in a mesh: blk: 512 (over z, y, x), uly: 2 (over core).
Axes of the slice: x: 8, y: 8, z: 8, core: 2. Of those that a mesh axis runs over, the one named last changes fastest.
Arguments:
- queries: bfloat16 [98304, 8192], P(('blk', 'uly')), may hold values from -300 to 300
- keys: bfloat16 [98304, 1024], P(('blk', 'uly')), may hold values from -4 to 4
- values: bfloat16 [98304, 1024], P(('blk', 'uly')), may hold values from -6 to 6
- doc_lengths: int32 [1024], replicated, may hold values from 1 to 384, as said below
Outputs:
- attention: bfloat16 [98304, 8192], P(('blk', 'uly'))
The draws below stay inside these ranges and needn't reach their ends.
Inputs may be any that keep to these rules, and one draw needn't show every extreme that they name: `doc_lengths`: every document has 1 to 384 tokens, the lengths sum to 98304, and some document has exactly 384 tokens.
All inputs are finite; a program needn't handle non-finite values.
Results may differ from the reference program's by a relative error of at most 0.003.
Values may be sent and summed in bfloat16 or wider, within the bound.
A program may use at most 32 MiB of HBM per device.

```python
import jax
import jax.numpy as jnp
from jax import lax

HEADS = 64
KV_HEADS = 8
HEAD_DIM = 128
TOK_DEV = 96
REACH = 2
BLOCK = 192
SEQ = 98304
MOST = 384
DOCS = 1024
N_BLK = 512
N_ULY = 2


def paired(key):
    base_key = jax.random.fold_in(key, 11)
    first_key, second_key = jax.random.split(base_key, 2)
    width_keys = KV_HEADS * HEAD_DIM
    width_queries = HEADS * HEAD_DIM
    keys_drawn = jax.random.truncated_normal(first_key, -4.0, 4.0, (SEQ, width_keys), jnp.float32)
    queries_drawn = jax.random.truncated_normal(second_key, -4.0, 4.0, (SEQ, width_queries), jnp.float32)
    return (queries_drawn, keys_drawn)


def draw_queries(key, part):
    return paired(key)[0].astype(jnp.bfloat16)


def draw_keys(key, part):
    return paired(key)[1].astype(jnp.bfloat16)


def draw_doc_lengths(key, part):
    offset_key, rank_key = jax.random.split(jax.random.fold_in(key, 23))
    opening = BLOCK // 2
    remaining = SEQ - opening - MOST
    stride = MOST // 2
    candidates = remaining - 1
    strata = (candidates + stride - 1) // stride
    stratum_ids = jnp.arange(strata, dtype=jnp.int32)
    limits = jnp.minimum(stride, candidates - stratum_ids * stride).astype(jnp.int32)
    offsets = jax.random.randint(offset_key, (strata,), 0, limits).astype(jnp.int32)
    positions = jnp.arange(candidates, dtype=jnp.int32)
    forced = (positions % stride == offsets[positions // stride]).astype(jnp.int32)
    ranks = jax.random.permutation(rank_key, candidates).astype(jnp.int32)
    score = forced * candidates + ranks
    order = jnp.argsort(-score, stable=True)[:DOCS - 3].astype(jnp.int32)
    cuts = jnp.sort(order + 1).astype(jnp.int32)
    bounds = jnp.concatenate([jnp.zeros((1,), jnp.int32), cuts, jnp.full((1,), remaining, jnp.int32)])
    gaps = (bounds[1:] - bounds[:-1]).astype(jnp.int32)
    leading = jnp.array([opening, MOST], jnp.int32)
    return jnp.concatenate([leading, gaps]).astype(jnp.int32)


def block_levels(stream_key, shape, shards, smallest, largest):
    factor_of, own = 1.0, jax.random.fold_in(stream_key, 6)
    for axis_at, blocks in shards:
        heights = jnp.exp(jax.random.uniform(jax.random.fold_in(own, axis_at), (blocks,), jnp.float32, smallest / len(shards), largest / len(shards)))
        factor_of = factor_of * jnp.repeat(heights, shape[axis_at] // blocks).reshape([-1 if axis == axis_at else 1 for axis in range(len(shape))])
    return factor_of


def gaussian(rng, shape, spread, limit, pieces=(), kind=jnp.bfloat16):
    gain = block_levels(rng, shape, pieces, -0.22, 0.18) if pieces else 1.0
    drawn = jax.random.normal(rng, shape, jnp.float32) * spread * gain
    return jnp.minimum(jnp.maximum(drawn, -limit), limit).astype(kind)


def setup_inputs(seed: int = 0) -> dict:
    splits = jax.random.split(jax.random.key(seed), 5)
    queries = draw_queries(jax.random.fold_in(splits[4], 71), 0)
    keys = draw_keys(jax.random.fold_in(splits[4], 71), 0)
    values = gaussian(splits[2], (SEQ, KV_HEADS * HEAD_DIM), 1.0, 6.0, ((0, 1024),))
    doc_lengths = draw_doc_lengths(jax.random.fold_in(splits[4], 71), 0)
    return dict(queries=queries, keys=keys, values=values, doc_lengths=doc_lengths)


MASKED = -1e30


def doc_index(positions, starts):
    return jnp.sum((positions[:, None] >= starts[None, :]).astype(jnp.int32), axis=1).astype(jnp.int32) - 1


def fold_block(running, grouped, query_pos, query_doc, key_block, value_block, anchor, starts):
    block_rows = key_block.shape[0]
    running_max, row_total, weighted = running
    key_pos = anchor * block_rows + jnp.arange(block_rows, dtype=jnp.int32)
    key_doc = doc_index(key_pos, starts)
    allowed = (key_doc[None, :] == query_doc[:, None]) & (key_pos[None, :] <= query_pos[:, None])
    heads_kv = key_block.shape[1] // HEAD_DIM
    key_heads = key_block.reshape(block_rows, heads_kv, HEAD_DIM).transpose(1, 0, 2).astype(jnp.float32)
    value_heads = value_block.reshape(block_rows, heads_kv, HEAD_DIM).transpose(1, 0, 2).astype(jnp.float32)
    scores = jnp.einsum("gqd,gkd->gqk", grouped.astype(jnp.float32), key_heads) * (HEAD_DIM ** -0.5)
    scores = jnp.where(allowed[None], scores, jnp.float32(MASKED))
    new_max = jnp.maximum(running_max, jnp.max(scores, axis=-1))
    rescale = jnp.exp(running_max - new_max)
    weights = jnp.exp(scores - new_max[..., None])
    row_total = row_total * rescale + jnp.sum(weights, axis=-1)
    rounded = lax.optimization_barrier(weights.astype(jnp.bfloat16)).astype(jnp.float32)
    weighted = weighted * rescale[..., None] + jnp.einsum("gqk,gkd->gqd", rounded, value_heads)
    return new_max, row_total, weighted


def reference(queries, keys, values, doc_lengths):
    block_rows = TOK_DEV * N_ULY
    group_size = HEADS // KV_HEADS
    query_rows = block_rows * group_size
    starts = (jnp.cumsum(doc_lengths).astype(jnp.int32) - doc_lengths).astype(jnp.int32)
    front_rows = REACH * block_rows
    keys_padded = jnp.pad(keys, ((front_rows, 0), (0, 0)))
    values_padded = jnp.pad(values, ((front_rows, 0), (0, 0)))

    def one_block(block_index):
        first_row = block_index * block_rows
        query_block = lax.dynamic_slice_in_dim(queries, first_row, block_rows, 0)
        grouped = query_block.reshape(block_rows, KV_HEADS, group_size, HEAD_DIM).transpose(1, 0, 2, 3)
        grouped = grouped.reshape(KV_HEADS, query_rows, HEAD_DIM)
        query_pos = first_row + jnp.arange(query_rows, dtype=jnp.int32) // group_size
        query_doc = doc_index(query_pos, starts)
        running = (jnp.full((KV_HEADS, query_rows), MASKED, jnp.float32),
                   jnp.zeros((KV_HEADS, query_rows), jnp.float32),
                   jnp.zeros((KV_HEADS, query_rows, HEAD_DIM), jnp.float32))
        for distance in range(REACH + 1):
            anchor = (block_index - distance).astype(jnp.int32)
            start_row = (front_rows + anchor * block_rows).astype(jnp.int32)
            key_block = lax.dynamic_slice_in_dim(keys_padded, start_row, block_rows, 0)
            value_block = lax.dynamic_slice_in_dim(values_padded, start_row, block_rows, 0)
            if distance == 0:
                running = fold_block(running, grouped, query_pos, query_doc, key_block, value_block, anchor, starts)
            else:
                last_doc = doc_index(jnp.reshape(anchor * block_rows + block_rows - 1, (1,)).astype(jnp.int32), starts)[0]
                needed = (anchor >= 0) & (last_doc == query_doc[0])

                def absorb(state_now, kb=key_block, vb=value_block, source=anchor):
                    return fold_block(state_now, grouped, query_pos, query_doc, kb, vb, source, starts)

                def keep_state(state_now):
                    return state_now

                running = lax.cond(needed, absorb, keep_state, running)
        result = running[2] / running[1][..., None]
        result = result.astype(jnp.bfloat16).reshape(KV_HEADS, block_rows, group_size, HEAD_DIM)
        return result.transpose(1, 0, 2, 3).reshape(block_rows, HEADS * HEAD_DIM)

    blocks_out = lax.map(one_block, jnp.arange(N_BLK, dtype=jnp.int32))
    return blocks_out.reshape(SEQ, HEADS * HEAD_DIM)
```

```python
import functools

import jax
import jax.numpy as jnp
from jax import lax
from jax.experimental import pallas as pl
from jax.experimental.pallas import tpu as pltpu
from jax.sharding import PartitionSpec as P

KV_HEADS = 8
GROUP = 8
JOINED = 4
HEAD_DIM = 128
TOK = 96
WIDE = GROUP * HEAD_DIM
PAD = 512
OWN = 4 * TOK
MASKED = -1e30
REACH = 2
COPIES = REACH * KV_HEADS
WINDOW = 4
LAG = 3
MESH = pl.DeviceIdType.MESH
EXP_SCALE = (HEAD_DIM ** -0.5) * 1.4426950408889634


def prefix_starts(lengths):
    lane = lax.broadcasted_iota(jnp.int32, lengths.shape, 1)
    row = lax.broadcasted_iota(jnp.int32, lengths.shape, 0)
    run = lengths
    shift = 1
    while shift < 128:
        run = run + jnp.where(lane >= shift, pltpu.roll(run, shift, 1), 0)
        shift *= 2
    totals = jnp.broadcast_to(jnp.sum(lengths, axis=1, keepdims=True), lengths.shape)
    base = jnp.zeros_like(lengths)
    for j in range(7):
        base = base + jnp.where(row > j, totals[j:j + 1, :], 0)
    return base + run - lengths


def fill_bias(lengths, me, bias):
    starts = prefix_starts(lengths)
    token = lax.broadcasted_iota(jnp.int32, (TOK, 128), 0) + me * TOK
    begin = jnp.zeros((TOK, 128), jnp.int32)
    for j in range(8):
        begin = jnp.maximum(begin, jnp.where(starts[j:j + 1, :] <= token, starts[j:j + 1, :], 0))
    begin = jnp.max(begin, axis=1, keepdims=True)
    key = lax.broadcasted_iota(jnp.int32, (TOK, PAD), 1) + (me - 4) * TOK
    query = lax.broadcasted_iota(jnp.int32, (TOK, PAD), 0) + me * TOK
    bias[...] = jnp.where((key >= begin) & (key <= query), 0.0, MASKED).astype(jnp.float32)


def attend(q, k, v, bias):
    scores = lax.dot_general(q, k, (((1,), (1,)), ((), ())), preferred_element_type=jnp.float32)
    scores = scores + bias
    top = jnp.max(scores, axis=1, keepdims=True)
    weights = jnp.exp2((scores - top) * EXP_SCALE)
    total = jnp.sum(weights, axis=1, keepdims=True)
    acc = jnp.dot(weights.astype(jnp.bfloat16), v, preferred_element_type=jnp.float32)
    return (acc / total).astype(jnp.bfloat16)


def kernel(n, doc_hbm, q_hbm, k_hbm, v_hbm, o_ref, docs, qbuf, kv, bias,
           doc_sem, q_sem, load_sem, send, recv, send_p, recv_p, send_r, recv_r):
    c = lax.axis_index("blk")
    core = lax.axis_index("uly")
    me = c * 2 + core

    def load(h, which, src):
        return pltpu.make_async_copy(
            src.at[:, h * HEAD_DIM:(h + 1) * HEAD_DIM], kv.at[h, which, pl.ds(OWN, TOK)], load_sem.at[h, which])

    for h in range(KV_HEADS):
        load(h, 0, k_hbm).start()
        load(h, 1, v_hbm).start()
    doc_copy = pltpu.make_async_copy(doc_hbm, docs, doc_sem)
    doc_copy.start()
    q_copy = pltpu.make_async_copy(q_hbm, qbuf, q_sem)
    q_copy.start()

    @pl.when(c < REACH)
    def _():
        for h in range(KV_HEADS):
            kv[h, :, :OWN, :] = jnp.zeros((2, OWN, HEAD_DIM), jnp.bfloat16)

    barrier = pltpu.get_barrier_semaphore()

    def greet(target):
        pl.semaphore_signal(barrier, inc=1, device_id=target, device_id_type=MESH)

    @pl.when(c > 0)
    def _():
        greet((c - 1, core))

    @pl.when(c < n - 1)
    def _():
        greet((c + 1, core))

    greet((c, 1 - core))
    pl.semaphore_wait(barrier, 1 + jnp.where(c > 0, 1, 0) + jnp.where(c < n - 1, 1, 0))

    def remote(h, src_row, dst_row, send_sem, recv_sem, target):
        return pltpu.make_async_remote_copy(
            src_ref=kv.at[h, :, pl.ds(src_row, TOK)], dst_ref=kv.at[h, :, pl.ds(dst_row, TOK)],
            send_sem=send_sem, recv_sem=recv_sem, device_id=target, device_id_type=MESH)

    def ahead(i):
        lap = i // KV_HEADS
        return remote(i % KV_HEADS, pl.multiple_of(OWN - 2 * TOK * lap, TOK), pl.multiple_of(2 * TOK - 2 * TOK * lap, TOK),
                      send.at[i], recv.at[i], (c + 1, core))

    def sends(i):
        return (c < n - 1) & (c >= i // KV_HEADS)

    def receives(i):
        return c >= 1 + i // KV_HEADS

    def partner_near(h):
        return remote(h, pl.multiple_of(OWN - 2 * TOK * core, TOK), 3 * TOK, send_p.at[h], recv_p.at[h], (c, 1 - core))

    def partner_far(h):
        return remote(h, pl.multiple_of(2 * TOK - 2 * TOK * core, TOK), TOK, send_r.at[h], recv_r.at[h], (c, 1 - core))

    for h in range(KV_HEADS):
        load(h, 0, k_hbm).wait()
        load(h, 1, v_hbm).wait()
        if h < WINDOW:
            @pl.when(sends(h))
            def _(h=h):
                ahead(h).start()

    for h in range(KV_HEADS):
        kv[h, :, 5 * TOK:, :] = jnp.zeros((2, PAD - 5 * TOK, HEAD_DIM), jnp.bfloat16)
    doc_copy.wait()
    fill_bias(docs[...], me, bias)
    q_copy.wait()

    def step(i, carry):
        @pl.when((i < COPIES) & sends(i))
        def _():
            ahead(i).wait_send()

        @pl.when((i + WINDOW < COPIES) & sends(i + WINDOW))
        def _():
            ahead(i + WINDOW).start()

        j = i - LAG

        @pl.when((j >= 0) & (j < COPIES) & receives(j))
        def _():
            ahead(j).wait_recv()

        @pl.when((j >= 0) & (j < KV_HEADS) & (c >= core))
        def _():
            partner_near(j).start()

        @pl.when((j >= KV_HEADS) & (j < COPIES) & (c >= 1 + core))
        def _():
            partner_far(j - KV_HEADS).start()

        h = i - LAG - 1 - KV_HEADS

        @pl.when(h >= 0)
        def _():
            @pl.when(c >= 1 - core)
            def _():
                partner_near(h).wait_recv()

            @pl.when(c >= 2 - core)
            def _():
                partner_far(h).wait_recv()

            k, v = kv[h, 0], kv[h, 1]
            wide_bias = jnp.concatenate([bias[...]] * JOINED, axis=0)
            for g in range(0, GROUP, JOINED):
                cols = [pl.ds(pl.multiple_of(h * WIDE + (g + t) * HEAD_DIM, HEAD_DIM), HEAD_DIM) for t in range(JOINED)]
                result = attend(jnp.concatenate([qbuf[:, at] for at in cols], axis=0), k, v, wide_bias)
                for t, at in enumerate(cols):
                    o_ref[:, at] = result[t * TOK:(t + 1) * TOK]

            @pl.when(c >= core)
            def _():
                partner_near(h).wait_send()

            @pl.when(c >= 1 + core)
            def _():
                partner_far(h).wait_send()

        return carry

    lax.fori_loop(0, COPIES + LAG + 1, step, 0)


def local(queries, keys, values, doc_lengths):
    n = lax.axis_size("blk")
    hbm = pl.BlockSpec(memory_space=pltpu.HBM)
    per_head = pltpu.SemaphoreType.DMA((KV_HEADS,))
    return pl.pallas_call(
        functools.partial(kernel, n),
        out_shape=pltpu.VMEM(queries.shape, jnp.bfloat16),
        in_specs=[hbm] * 4,
        out_specs=pl.BlockSpec(memory_space=pltpu.VMEM),
        scratch_shapes=[
            pltpu.VMEM((8, 128), jnp.int32),
            pltpu.VMEM(queries.shape, jnp.bfloat16),
            pltpu.VMEM((KV_HEADS, 2, PAD, HEAD_DIM), jnp.bfloat16),
            pltpu.VMEM((TOK, PAD), jnp.float32),
            pltpu.SemaphoreType.DMA,
            pltpu.SemaphoreType.DMA,
            pltpu.SemaphoreType.DMA((KV_HEADS, 2)),
        ] + [pltpu.SemaphoreType.DMA((COPIES,))] * 2 + [per_head] * 4,
        compiler_params=pltpu.CompilerParams(
            collective_id=0, has_side_effects=True, vmem_limit_bytes=32 * 1024 * 1024),
    )(*[pltpu.with_memory_space_constraint(x, pltpu.HBM) for x in (doc_lengths.reshape(8, 128), queries, keys, values)])


def solution(mesh):
    in_specs = (P(("blk", "uly"), None), P(("blk", "uly"), None), P(("blk", "uly"), None), P())
    out_specs = P(("blk", "uly"), None)
    return jax.shard_map(local, mesh=mesh, in_specs=in_specs, out_specs=out_specs, check_vma=False)
```

```python
import functools

import jax
import jax.numpy as jnp
from jax import lax
from jax.experimental import pallas as pl
from jax.experimental.pallas import tpu as pltpu
from jax.sharding import PartitionSpec as P

KV_HEADS = 8
GROUP = 8
JOINED = 4
HEAD_DIM = 128
TOK = 96
WIDE = GROUP * HEAD_DIM
PAD = 32
WINDOW = 512
HALF = WINDOW // 2
OWN = PAD + 4 * TOK
MASKED = -1e30
REACH = 2
COPIES = REACH * KV_HEADS
ROW = 8
PLANE = 8 * ROW
MESH = pl.DeviceIdType.MESH
EXP_SCALE = (HEAD_DIM ** -0.5) * 1.4426950408889634


def prefix_starts(lengths):
    lane = lax.broadcasted_iota(jnp.int32, lengths.shape, 1)
    row = lax.broadcasted_iota(jnp.int32, lengths.shape, 0)
    run = lengths
    shift = 1
    while shift < 128:
        run = run + jnp.where(lane >= shift, pltpu.roll(run, shift, 1), 0)
        shift *= 2
    totals = jnp.broadcast_to(jnp.sum(lengths, axis=1, keepdims=True), lengths.shape)
    base = jnp.zeros_like(lengths)
    for j in range(7):
        base = base + jnp.where(row > j, totals[j:j + 1, :], 0)
    return base + run - lengths


def fill_bias(lengths, me, bias):
    starts = prefix_starts(lengths)
    token = lax.broadcasted_iota(jnp.int32, (TOK, 128), 0) + me * TOK
    begin = jnp.zeros((TOK, 128), jnp.int32)
    for j in range(8):
        begin = jnp.maximum(begin, jnp.where(starts[j:j + 1, :] <= token, starts[j:j + 1, :], 0))
    begin = jnp.max(begin, axis=1, keepdims=True)
    place = lax.broadcasted_iota(jnp.int32, (TOK, WINDOW), 1)
    key = place + (me * TOK - OWN)
    query = lax.broadcasted_iota(jnp.int32, (TOK, WINDOW), 0) + me * TOK
    bias[...] = jnp.where((place >= PAD) & (key >= begin) & (key <= query), 0.0, MASKED).astype(jnp.float32)


def twice(x):
    return jnp.concatenate([x, x], axis=1)


def masked_scores(q, k, bias):
    scores = lax.dot_general(q, k, (((1,), (1,)), ((), ())), preferred_element_type=jnp.float32)
    return scores + jnp.concatenate([bias] * JOINED, axis=0)


def row_max(scores):
    return jnp.broadcast_to(jnp.max(scores, axis=1, keepdims=True), (scores.shape[0], HEAD_DIM))


def weighted(scores, top, v):
    weights = jnp.exp2((scores - twice(top)) * EXP_SCALE)
    return jnp.dot(weights.astype(jnp.bfloat16), v, preferred_element_type=jnp.float32)


def with_ones(v):
    return jnp.concatenate([v, jnp.ones_like(v)], axis=1)


def kernel(n, doc_hbm, q_hbm, k_hbm, v_hbm, o_ref, docs, qbuf, kv, held, bias, sums, tops,
           doc_sem, q_sem, load_sem, send, recv, relay_out, relay_in, send_p, recv_p, send_r, recv_r):
    c = lax.axis_index("blk")
    core = lax.axis_index("uly")
    me = c * 2 + core
    relays = (c % ROW == ROW - 1) & (c < PLANE)
    origin = jnp.where(c < ROW, PLANE - 1, c - ROW)
    relay = jnp.where(c < PLANE - ROW, c + ROW, ROW - 1)
    relayed = (c % ROW == 0) & (c > 0) & (c <= PLANE)
    before = jnp.where(relayed, jnp.where(c < PLANE, c + ROW - 1, ROW - 1), c - 1)
    has_next = c < n - 1

    def load(h, which, src):
        return pltpu.make_async_copy(
            src.at[:, h * HEAD_DIM:(h + 1) * HEAD_DIM], kv.at[h, which, pl.ds(OWN, TOK)], load_sem.at[h, which])

    for h in range(KV_HEADS):
        load(h, 0, k_hbm).start()
        load(h, 1, v_hbm).start()
    doc_copy = pltpu.make_async_copy(doc_hbm, docs, doc_sem)
    doc_copy.start()
    q_copy = pltpu.make_async_copy(q_hbm, qbuf, q_sem)
    q_copy.start()

    @pl.when(c < REACH)
    def _():
        for h in range(KV_HEADS):
            kv[h, :, PAD:OWN, :] = jnp.zeros((2, OWN - PAD, HEAD_DIM), jnp.bfloat16)

    barrier = pltpu.get_barrier_semaphore()

    def greet(target):
        pl.semaphore_signal(barrier, inc=1, device_id=target, device_id_type=MESH)

    @pl.when(c > 0)
    def _():
        greet((before, core))

    @pl.when(relays)
    def _():
        greet((origin, core))

    @pl.when(c >= 1 - core)
    def _():
        greet((c, 1 - core))

    pl.semaphore_wait(
        barrier, jnp.where(c >= core, 1, 0) + jnp.where(has_next, 1, 0) + jnp.where(relays, 1, 0))

    def remote(src, dst, send_sem, recv_sem, target):
        return pltpu.make_async_remote_copy(
            src_ref=src, dst_ref=dst, send_sem=send_sem, recv_sem=recv_sem, device_id=target, device_id_type=MESH)

    def rows(h, row):
        return kv.at[h, :, pl.ds(row, TOK)]

    def chunk(i):
        lap = i // KV_HEADS
        src = pl.multiple_of(OWN - 2 * TOK * lap, PAD)
        return rows(i % KV_HEADS, src), rows(i % KV_HEADS, pl.multiple_of(src - 2 * TOK, PAD))

    def ahead(i):
        src, dst = chunk(i)
        return remote(src, dst, send.at[i], recv.at[i], (c + 1, core))

    def to_relay(i):
        return remote(chunk(i)[0], held.at[i], send.at[i], relay_in.at[i], (relay, core))

    def from_relay(i):
        return remote(held.at[i], chunk(i)[1], relay_out.at[i], recv.at[i], (origin + 1, core))

    def start_ahead(i):
        @pl.when(jnp.logical_not(relays))
        def _():
            ahead(i).start()

        @pl.when(relays)
        def _():
            to_relay(i).start()

    def across(h, src, dst, send_sem, recv_sem):
        return remote(rows(h, PAD + src * TOK), rows(h, PAD + dst * TOK), send_sem.at[h], recv_sem.at[h], (c, 1 - core))

    def own_across(h):
        return across(h, 4, 3, send_p, recv_p)

    def near_across(h):
        return across(h, 2, 3, send_p, recv_p)

    def mid_across(h):
        return across(h, 2, 1, send_r, recv_r)

    def far_across(h):
        return across(h, 0, 1, send_r, recv_r)

    for h in range(KV_HEADS):
        load(h, 0, k_hbm).wait()
        load(h, 1, v_hbm).wait()

        @pl.when(has_next)
        def _(h=h):
            start_ahead(h)

        @pl.when(core == 0)
        def _(h=h):
            own_across(h).start()

    for h in range(KV_HEADS):
        kv[h, :, :PAD, :] = jnp.zeros((2, PAD, HEAD_DIM), jnp.bfloat16)
    doc_copy.wait()
    fill_bias(docs[...], me, bias)
    q_copy.wait()

    def step(i, carry):
        @pl.when(relays & (i < COPIES))
        def _():
            from_relay_in(i)
            from_relay(i).start()

        @pl.when((c >= 1) & (i < KV_HEADS))
        def _():
            ahead(i).wait_recv()

            @pl.when(has_next)
            def _():
                start_ahead(i + KV_HEADS)

            @pl.when(core == 0)
            def _():
                mid_across(i).start()

            @pl.when(core == 1)
            def _():
                near_across(i).start()

        @pl.when((c >= 2) & (i >= KV_HEADS) & (i < COPIES))
        def _():
            ahead(i).wait_recv()

            @pl.when(core == 1)
            def _():
                far_across(i - KV_HEADS).start()

        @pl.when((i >= 1) & (i <= KV_HEADS))
        def _():
            h = i - 1

            @pl.when(c >= 1 - core)
            def _():
                own_across(h).wait_recv()

            k, v = kv[h, 0, HALF:], with_ones(kv[h, 1, HALF:])
            for g in range(0, GROUP, JOINED):
                scores = masked_scores(joined_queries(h, g), k, bias[:, HALF:])
                top = row_max(scores)
                at = pl.ds(g * TOK, JOINED * TOK)
                tops[h, at, :] = top
                sums[h, at, :] = weighted(scores, top, v)

        @pl.when(i > KV_HEADS)
        def _():
            h = i - 1 - KV_HEADS

            @pl.when(c >= 2 - core)
            def _():
                far_across(h).wait_recv()

            k, v = kv[h, 0, :HALF], with_ones(kv[h, 1, :HALF])
            for g in range(0, GROUP, JOINED):
                scores = masked_scores(joined_queries(h, g), k, bias[:, :HALF])
                at = pl.ds(g * TOK, JOINED * TOK)
                near_top = tops[h, at, :]
                top = jnp.maximum(near_top, row_max(scores))
                rescale = jnp.exp2((near_top - top) * EXP_SCALE)
                total = sums[h, at, :] * twice(rescale) + weighted(scores, top, v)
                result = (total[:, :HEAD_DIM] / total[:, HEAD_DIM:]).astype(jnp.bfloat16)
                for t in range(JOINED):
                    o_ref[:, columns(h, g + t)] = result[t * TOK:(t + 1) * TOK]

        return carry

    def columns(h, g):
        return pl.ds(pl.multiple_of(h * WIDE + g * HEAD_DIM, HEAD_DIM), HEAD_DIM)

    def joined_queries(h, g):
        return jnp.concatenate([qbuf[:, columns(h, g + t)] for t in range(JOINED)], axis=0)

    def from_relay_in(i):
        remote(held.at[i], held.at[i], relay_out.at[i], relay_in.at[i], (origin + 1, core)).wait_recv()

    lax.fori_loop(0, COPIES + 1, step, 0)

    def drain(i, carry):
        @pl.when(has_next & (c >= i // KV_HEADS))
        def _():
            ahead(i).wait_send()

        @pl.when(relays)
        def _():
            from_relay(i).wait_send()

        @pl.when((i < KV_HEADS) & (c >= core))
        def _():
            own_across(i).wait_send()

        @pl.when((i >= KV_HEADS) & (c >= 1 + core))
        def _():
            far_across(i - KV_HEADS).wait_send()

        return carry

    lax.fori_loop(0, COPIES, drain, 0)


def local(queries, keys, values, doc_lengths):
    n = lax.axis_size("blk")
    hbm = pl.BlockSpec(memory_space=pltpu.HBM)
    per_head = pltpu.SemaphoreType.DMA((KV_HEADS,))
    return pl.pallas_call(
        functools.partial(kernel, n),
        out_shape=pltpu.VMEM(queries.shape, jnp.bfloat16),
        in_specs=[hbm] * 4,
        out_specs=pl.BlockSpec(memory_space=pltpu.VMEM),
        scratch_shapes=[
            pltpu.VMEM((8, 128), jnp.int32),
            pltpu.VMEM(queries.shape, jnp.bfloat16),
            pltpu.VMEM((KV_HEADS, 2, WINDOW, HEAD_DIM), jnp.bfloat16),
            pltpu.VMEM((COPIES, 2, TOK, HEAD_DIM), jnp.bfloat16),
            pltpu.VMEM((TOK, WINDOW), jnp.float32),
            pltpu.VMEM((KV_HEADS, GROUP * TOK, 2 * HEAD_DIM), jnp.float32),
            pltpu.VMEM((KV_HEADS, GROUP * TOK, HEAD_DIM), jnp.float32),
            pltpu.SemaphoreType.DMA,
            pltpu.SemaphoreType.DMA,
            pltpu.SemaphoreType.DMA((KV_HEADS, 2)),
        ] + [pltpu.SemaphoreType.DMA((COPIES,))] * 4 + [per_head] * 4,
        compiler_params=pltpu.CompilerParams(
            collective_id=0, has_side_effects=True, vmem_limit_bytes=32 * 1024 * 1024),
    )(*[pltpu.with_memory_space_constraint(x, pltpu.HBM) for x in (doc_lengths.reshape(8, 128), queries, keys, values)])


def solution(mesh):
    in_specs = (P(("blk", "uly"), None), P(("blk", "uly"), None), P(("blk", "uly"), None), P())
    out_specs = P(("blk", "uly"), None)
    return jax.shard_map(local, mesh=mesh, in_specs=in_specs, out_specs=out_specs, check_vma=False)
```

```python
import functools

import jax
import jax.numpy as jnp
from jax import lax
from jax.experimental import pallas as pl
from jax.experimental.pallas import tpu as pltpu
from jax.sharding import PartitionSpec as P

KV_HEADS = 8
GROUP = 8
JOINED = 4
HEAD_DIM = 128
TOK = 96
WIDE = GROUP * HEAD_DIM
PAD = 32
WINDOW = 512
HALF = WINDOW // 2
OWN = PAD + 4 * TOK
MASKED = -1e30
REACH = 2
COPIES = REACH * KV_HEADS
ROW = 8
PLANE = 8 * ROW
MESH = pl.DeviceIdType.MESH
EXP_SCALE = (HEAD_DIM ** -0.5) * 1.4426950408889634


def prefix_starts(lengths):
    lane = lax.broadcasted_iota(jnp.int32, lengths.shape, 1)
    row = lax.broadcasted_iota(jnp.int32, lengths.shape, 0)
    run = lengths
    shift = 1
    while shift < 128:
        run = run + jnp.where(lane >= shift, pltpu.roll(run, shift, 1), 0)
        shift *= 2
    totals = jnp.broadcast_to(jnp.sum(lengths, axis=1, keepdims=True), lengths.shape)
    base = jnp.zeros_like(lengths)
    for j in range(7):
        base = base + jnp.where(row > j, totals[j:j + 1, :], 0)
    return base + run - lengths


def fill_bias(lengths, me, bias):
    starts = prefix_starts(lengths)
    token = lax.broadcasted_iota(jnp.int32, (TOK, 128), 0) + me * TOK
    begin = jnp.zeros((TOK, 128), jnp.int32)
    for j in range(8):
        begin = jnp.maximum(begin, jnp.where(starts[j:j + 1, :] <= token, starts[j:j + 1, :], 0))
    begin = jnp.max(begin, axis=1, keepdims=True)
    place = lax.broadcasted_iota(jnp.int32, (TOK, WINDOW), 1)
    key = place + (me * TOK - OWN)
    query = lax.broadcasted_iota(jnp.int32, (TOK, WINDOW), 0) + me * TOK
    bias[...] = jnp.where((place >= PAD) & (key >= begin) & (key <= query), 0.0, MASKED).astype(jnp.float32)


def twice(x):
    return jnp.concatenate([x, x], axis=1)


def masked_scores(q, k, bias):
    scores = lax.dot_general(q, k, (((1,), (1,)), ((), ())), preferred_element_type=jnp.float32)
    return scores + jnp.concatenate([bias] * JOINED, axis=0)


def row_max(scores):
    return jnp.broadcast_to(jnp.max(scores, axis=1, keepdims=True), (scores.shape[0], HEAD_DIM))


def weighted(scores, top, v):
    weights = jnp.exp2((scores - twice(top)) * EXP_SCALE)
    return jnp.dot(weights.astype(jnp.bfloat16), v, preferred_element_type=jnp.float32)


def with_ones(v):
    return jnp.concatenate([v, jnp.ones_like(v)], axis=1)


def kernel(n, doc_hbm, q_hbm, k_hbm, v_hbm, o_ref, docs, qbuf, kv, held, bias, sums, tops,
           doc_sem, q_sem, load_sem, send, recv, relay_out, relay_in, send_p, recv_p, send_r, recv_r):
    c = lax.axis_index("blk")
    core = lax.axis_index("uly")
    me = c * 2 + core
    relays = (c % ROW == ROW - 1) & (c < PLANE)
    origin = jnp.where(c < ROW, PLANE - 1, c - ROW)
    relay = jnp.where(c < PLANE - ROW, c + ROW, ROW - 1)
    relayed = (c % ROW == 0) & (c > 0) & (c <= PLANE)
    before = jnp.where(relayed, jnp.where(c < PLANE, c + ROW - 1, ROW - 1), c - 1)
    has_next = c < n - 1

    def load(h, which, src):
        return pltpu.make_async_copy(
            src.at[:, h * HEAD_DIM:(h + 1) * HEAD_DIM], kv.at[h, which, pl.ds(OWN, TOK)], load_sem.at[h, which])

    for h in range(KV_HEADS):
        load(h, 0, k_hbm).start()
        load(h, 1, v_hbm).start()
    doc_copy = pltpu.make_async_copy(doc_hbm, docs, doc_sem)
    doc_copy.start()
    q_copy = pltpu.make_async_copy(q_hbm, qbuf, q_sem)
    q_copy.start()

    @pl.when(c < REACH)
    def _():
        for h in range(KV_HEADS):
            kv[h, :, PAD:OWN, :] = jnp.zeros((2, OWN - PAD, HEAD_DIM), jnp.bfloat16)

    barrier = pltpu.get_barrier_semaphore()

    def greet(target):
        pl.semaphore_signal(barrier, inc=1, device_id=target, device_id_type=MESH)

    @pl.when(c > 0)
    def _():
        greet((before, core))

    @pl.when(relays)
    def _():
        greet((origin, core))

    @pl.when(c >= 1 - core)
    def _():
        greet((c, 1 - core))

    pl.semaphore_wait(
        barrier, jnp.where(c >= core, 1, 0) + jnp.where(has_next, 1, 0) + jnp.where(relays, 1, 0))

    def remote(src, dst, send_sem, recv_sem, target):
        return pltpu.make_async_remote_copy(
            src_ref=src, dst_ref=dst, send_sem=send_sem, recv_sem=recv_sem, device_id=target, device_id_type=MESH)

    def rows(h, row):
        return kv.at[h, :, pl.ds(row, TOK)]

    def chunk(i):
        lap = i // KV_HEADS
        src = pl.multiple_of(OWN - 2 * TOK * lap, PAD)
        return rows(i % KV_HEADS, src), rows(i % KV_HEADS, pl.multiple_of(src - 2 * TOK, PAD))

    def ahead(i):
        src, dst = chunk(i)
        return remote(src, dst, send.at[i], recv.at[i], (c + 1, core))

    def to_relay(i):
        src = chunk(i)[0]
        return [remote(src.at[t], held.at[i, t], send.at[i], relay_in.at[i, t], (relay, core)) for t in range(2)]

    def from_relay(i):
        dst = chunk(i)[1]
        return [remote(held.at[i, t], dst.at[t], relay_out.at[i], recv.at[i], (origin + 1, core)) for t in range(2)]

    def start_ahead(i):
        @pl.when(jnp.logical_not(relays))
        def _():
            ahead(i).start()

        @pl.when(relays)
        def _():
            for copy in to_relay(i):
                copy.start()

    def across(h, src, dst, send_sem, recv_sem):
        return remote(rows(h, PAD + src * TOK), rows(h, PAD + dst * TOK), send_sem.at[h], recv_sem.at[h], (c, 1 - core))

    def own_across(h):
        return across(h, 4, 3, send_p, recv_p)

    def near_across(h):
        return across(h, 2, 3, send_p, recv_p)

    def mid_across(h):
        return across(h, 2, 1, send_r, recv_r)

    def far_across(h):
        return across(h, 0, 1, send_r, recv_r)

    for h in range(KV_HEADS):
        load(h, 0, k_hbm).wait()
        load(h, 1, v_hbm).wait()

        @pl.when(has_next)
        def _(h=h):
            start_ahead(h)

        @pl.when(core == 0)
        def _(h=h):
            own_across(h).start()

    for h in range(KV_HEADS):
        kv[h, :, :PAD, :] = jnp.zeros((2, PAD, HEAD_DIM), jnp.bfloat16)
    doc_copy.wait()
    fill_bias(docs[...], me, bias)
    q_copy.wait()

    def columns(h, g):
        return pl.ds(pl.multiple_of(h * WIDE + g * HEAD_DIM, HEAD_DIM), HEAD_DIM)

    def joined_queries(h, g):
        return jnp.concatenate([qbuf[:, columns(h, g + t)] for t in range(JOINED)], axis=0)

    def receive(i):
        @pl.when((c >= 1) & (i < KV_HEADS))
        def _():
            ahead(i).wait_recv()

            @pl.when(has_next)
            def _():
                start_ahead(i + KV_HEADS)

            @pl.when(core == 0)
            def _():
                mid_across(i).start()

            @pl.when(core == 1)
            def _():
                near_across(i).start()

        @pl.when((c >= 2) & (i >= KV_HEADS) & (core == 1))
        def _():
            ahead(i).wait_recv()
            far_across(i - KV_HEADS).start()

        @pl.when(relays)
        def _():
            for arrived, copy in zip(into_relay(i), from_relay(i)):
                arrived.wait_recv()
                copy.start()

    def into_relay(i):
        return [remote(held.at[i, t], held.at[i, t], relay_out.at[i], relay_in.at[i, t], (origin + 1, core)) for t in range(2)]

    def near_half(heads):
        for h in heads:
            @pl.when(c >= 1 - core)
            def _(h=h):
                own_across(h).wait_recv()

        for h in heads:
            k, v = kv[h, 0, HALF:], with_ones(kv[h, 1, HALF:])
            for g in range(0, GROUP, JOINED):
                scores = masked_scores(joined_queries(h, g), k, bias[:, HALF:])
                top = row_max(scores)
                at = pl.ds(g * TOK, JOINED * TOK)
                tops[h, at, :] = top
                sums[h, at, :] = weighted(scores, top, v)

    def far_half(heads):
        for h in heads:
            @pl.when((c >= 2) & (core == 0))
            def _(h=h):
                ahead(h + KV_HEADS).wait_recv()

            @pl.when(c >= 2 - core)
            def _(h=h):
                far_across(h).wait_recv()

        for h in heads:
            k, v = kv[h, 0, :HALF], with_ones(kv[h, 1, :HALF])
            for g in range(0, GROUP, JOINED):
                scores = masked_scores(joined_queries(h, g), k, bias[:, :HALF])
                at = pl.ds(g * TOK, JOINED * TOK)
                near_top = tops[h, at, :]
                top = jnp.maximum(near_top, row_max(scores))
                rescale = jnp.exp2((near_top - top) * EXP_SCALE)
                total = sums[h, at, :] * twice(rescale) + weighted(scores, top, v)
                result = (total[:, :HEAD_DIM] / total[:, HEAD_DIM:]).astype(jnp.bfloat16)
                for t in range(JOINED):
                    o_ref[:, columns(h, g + t)] = result[t * TOK:(t + 1) * TOK]

    def step(i, carry):
        @pl.when(i < COPIES)
        def _():
            receive(i)

        @pl.when((i >= 2) & (i <= KV_HEADS) & (i % 2 == 0))
        def _():
            near_half((i - 2, i - 1))

        @pl.when(i > KV_HEADS)
        def _():
            far_half((i - 1 - KV_HEADS,))

        return carry

    lax.fori_loop(0, COPIES + 1, step, 0)

    def drain(i, carry):
        @pl.when(has_next & (c >= i // KV_HEADS))
        def _():
            ahead(i).wait_send()

        @pl.when(relays)
        def _():
            for copy in from_relay(i):
                copy.wait_send()

        @pl.when((i < KV_HEADS) & (c >= core))
        def _():
            own_across(i).wait_send()

        @pl.when((i >= KV_HEADS) & (c >= 1 + core))
        def _():
            far_across(i - KV_HEADS).wait_send()

        return carry

    lax.fori_loop(0, COPIES, drain, 0)


def local(queries, keys, values, doc_lengths):
    n = lax.axis_size("blk")
    hbm = pl.BlockSpec(memory_space=pltpu.HBM)
    per_head = pltpu.SemaphoreType.DMA((KV_HEADS,))
    return pl.pallas_call(
        functools.partial(kernel, n),
        out_shape=pltpu.VMEM(queries.shape, jnp.bfloat16),
        in_specs=[hbm] * 4,
        out_specs=pl.BlockSpec(memory_space=pltpu.VMEM),
        scratch_shapes=[
            pltpu.VMEM((8, 128), jnp.int32),
            pltpu.VMEM(queries.shape, jnp.bfloat16),
            pltpu.VMEM((KV_HEADS, 2, WINDOW, HEAD_DIM), jnp.bfloat16),
            pltpu.VMEM((COPIES, 2, TOK, HEAD_DIM), jnp.bfloat16),
            pltpu.VMEM((TOK, WINDOW), jnp.float32),
            pltpu.VMEM((KV_HEADS, GROUP * TOK, 2 * HEAD_DIM), jnp.float32),
            pltpu.VMEM((KV_HEADS, GROUP * TOK, HEAD_DIM), jnp.float32),
            pltpu.SemaphoreType.DMA,
            pltpu.SemaphoreType.DMA,
            pltpu.SemaphoreType.DMA((KV_HEADS, 2)),
        ] + [pltpu.SemaphoreType.DMA((COPIES,))] * 3 + [pltpu.SemaphoreType.DMA((COPIES, 2))] + [per_head] * 4,
        compiler_params=pltpu.CompilerParams(
            collective_id=0, has_side_effects=True, vmem_limit_bytes=32 * 1024 * 1024),
    )(*[pltpu.with_memory_space_constraint(x, pltpu.HBM) for x in (doc_lengths.reshape(8, 128), queries, keys, values)])


def solution(mesh):
    in_specs = (P(("blk", "uly"), None), P(("blk", "uly"), None), P(("blk", "uly"), None), P())
    out_specs = P(("blk", "uly"), None)
    return jax.shard_map(local, mesh=mesh, in_specs=in_specs, out_specs=out_specs, check_vma=False)
```
